128 devices in a mesh: ep: 64 (over z, y, x), dp: 2 (over core).
Axes of the slice: x: 4, y: 4, z: 4, core: 2. Of those that a mesh axis runs over, the one named last changes fastest.
Arguments:
- act_in: bfloat16 [98304, 448], P(('ep', 'dp'))
- grad_out: bfloat16 [98304, 448], P(('ep', 'dp'))
- slot_ids: int32 [2, 98304, 2], P(None, ('ep', 'dp'))
- gate_vals: float32 [2, 98304, 2], P(None, ('ep', 'dp'))
- w_dense: bfloat16 [2, 448, 448], replicated
- w_gate: bfloat16 [2, 128, 448, 304], P(None, 'ep')
- w_up: bfloat16 [2, 128, 448, 304], P(None, 'ep')
- w_down: bfloat16 [2, 128, 304, 448], P(None, 'ep')
- ws_gate: bfloat16 [2, 448, 304], replicated
- ws_up: bfloat16 [2, 448, 304], replicated
- ws_down: bfloat16 [2, 304, 448], replicated
Outputs:
- output 1: bfloat16 [98304, 448], P(('ep', 'dp'))
- output 2: bfloat16 [2, 448, 448], replicated
- output 3: bfloat16 [2, 128, 448, 304], P(None, 'ep')
- output 4: bfloat16 [2, 128, 448, 304], P(None, 'ep')
- output 5: bfloat16 [2, 128, 304, 448], P(None, 'ep')
- output 6: bfloat16 [2, 448, 304], replicated
- output 7: bfloat16 [2, 448, 304], replicated
- output 8: bfloat16 [2, 304, 448], replicated
All inputs are finite; a program needn't handle non-finite values.
Results may differ from the reference program's by a relative error of at most 0.02.
Values are sent between devices in bfloat16 or wider.
A program may use at most 1 GiB of HBM per device.

```python
import functools
import jax
import jax.numpy as jnp
from jax import lax

D = 448
FF = 304
FS = 304
EXPERTS = 128
TOP = 2
TOKENS = 768
EP = 64
DP = 2
LAYERS = 2

NUM_DEV = EP * DP
CAP = 2 * TOKENS * TOP // EXPERTS
ROWS = NUM_DEV * TOKENS


def draw_slots(key):
    key_tok, key_exp = jax.random.split(key)
    mean_load = TOKENS * TOP // EXPERTS
    order = jax.random.permutation(key_tok, TOKENS)
    position = jnp.arange(TOP, dtype=jnp.int32)[None, :] * TOKENS + order[:, None]
    group = position // (4 * mean_load)
    rest = position % (4 * mean_load)
    first = 2 * mean_load
    second = first + mean_load // 2
    third = second + mean_load // 2
    within = (rest >= first).astype(jnp.int32) + (rest >= second).astype(jnp.int32) + (rest >= third).astype(jnp.int32)
    start = jnp.where(rest >= third, third, jnp.where(rest >= second, second, jnp.where(rest >= first, first, 0)))
    expert_perm = jax.random.permutation(key_exp, EXPERTS)
    expert = expert_perm[group * 4 + within]
    return (expert * CAP + rest - start).astype(jnp.int32)


def setup_inputs(seed: int = 0) -> dict:
    keys = jax.random.split(jax.random.key(seed), 12)
    slot_keys = jax.random.split(keys[0], LAYERS * NUM_DEV)
    slot_ids = jax.vmap(draw_slots)(slot_keys).reshape(LAYERS, ROWS, TOP)
    gate_vals = jax.random.uniform(keys[1], (LAYERS, ROWS, TOP), jnp.float32, 0.5, 1.5) / TOP
    act_in = jax.random.normal(keys[2], (ROWS, D), jnp.float32).astype(jnp.bfloat16)
    grad_out = jax.random.normal(keys[3], (ROWS, D), jnp.float32).astype(jnp.bfloat16)
    w_dense = (jax.random.normal(keys[4], (LAYERS, D, D), jnp.float32) * D ** -0.5).astype(jnp.bfloat16)
    w_gate = (jax.random.normal(keys[5], (LAYERS, EXPERTS, D, FF), jnp.float32) * D ** -0.5).astype(jnp.bfloat16)
    w_up = (jax.random.normal(keys[6], (LAYERS, EXPERTS, D, FF), jnp.float32) * D ** -0.5).astype(jnp.bfloat16)
    w_down = (jax.random.normal(keys[7], (LAYERS, EXPERTS, FF, D), jnp.float32) * FF ** -0.5).astype(jnp.bfloat16)
    ws_gate = (jax.random.normal(keys[8], (LAYERS, D, FS), jnp.float32) * D ** -0.5).astype(jnp.bfloat16)
    ws_up = (jax.random.normal(keys[9], (LAYERS, D, FS), jnp.float32) * D ** -0.5).astype(jnp.bfloat16)
    ws_down = (jax.random.normal(keys[10], (LAYERS, FS, D), jnp.float32) * FS ** -0.5).astype(jnp.bfloat16)
    return {"act_in": act_in, "grad_out": grad_out, "slot_ids": slot_ids, "gate_vals": gate_vals, "w_dense": w_dense, "w_gate": w_gate, "w_up": w_up, "w_down": w_down, "ws_gate": ws_gate, "ws_up": ws_up, "ws_down": ws_down}


def expert_block(args, w_gate32, w_up32, w_down32):
    mixed_loc, slot_loc, gate_loc = args
    slot_flat = slot_loc.reshape(TOKENS * TOP)
    copies = jnp.broadcast_to(mixed_loc[:, None, :], (TOKENS, TOP, D)).reshape(TOKENS * TOP, D)
    dispatched = jnp.zeros((EXPERTS * CAP, D), mixed_loc.dtype).at[slot_flat].set(copies)
    dispatched = dispatched.reshape(EXPERTS, CAP, D).astype(jnp.float32)
    a_one = jnp.einsum("ecd,edf->ecf", dispatched, w_gate32)
    a_three = jnp.einsum("ecd,edf->ecf", dispatched, w_up32)
    hidden = (jax.nn.silu(a_one) * a_three).astype(jnp.bfloat16)
    exp_out = jnp.einsum("ecf,efd->ecd", hidden.astype(jnp.float32), w_down32).astype(jnp.bfloat16)
    picked = exp_out.reshape(EXPERTS * CAP, D)[slot_flat].reshape(TOKENS, TOP, D)
    return jnp.sum(gate_loc[:, :, None] * picked.astype(jnp.float32), axis=1)


def moe_layer(act, layer_in):
    w_dense, w_gate, w_up, w_down, ws_gate, ws_up, ws_down, slot_ids, gate_vals = layer_in
    dense_pre = jnp.dot(act, w_dense, preferred_element_type=jnp.float32)
    mixed = (act.astype(jnp.float32) + dense_pre).astype(jnp.bfloat16)
    s_one = jnp.dot(mixed, ws_gate, preferred_element_type=jnp.float32)
    s_three = jnp.dot(mixed, ws_up, preferred_element_type=jnp.float32)
    shared_hidden = (jax.nn.silu(s_one) * s_three).astype(jnp.bfloat16)
    shared_out = jnp.dot(shared_hidden, ws_down, preferred_element_type=jnp.float32)
    block = jax.checkpoint(functools.partial(expert_block, w_gate32=w_gate.astype(jnp.float32), w_up32=w_up.astype(jnp.float32), w_down32=w_down.astype(jnp.float32)))
    routed = lax.map(block, (mixed.reshape(NUM_DEV, TOKENS, D), slot_ids.reshape(NUM_DEV, TOKENS, TOP), gate_vals.reshape(NUM_DEV, TOKENS, TOP)))
    routed = routed.reshape(ROWS, D)
    new_act = (mixed.astype(jnp.float32) + routed + shared_out).astype(jnp.bfloat16)
    return new_act, None


def reference(act_in, grad_out, slot_ids, gate_vals, w_dense, w_gate, w_up, w_down, ws_gate, ws_up, ws_down):
    def forward(act, dense_all, gate_all, up_all, down_all, sgate_all, sup_all, sdown_all):
        final, _ = lax.scan(moe_layer, act, (dense_all, gate_all, up_all, down_all, sgate_all, sup_all, sdown_all, slot_ids, gate_vals))
        return final
    _, pullback = jax.vjp(forward, act_in, w_dense, w_gate, w_up, w_down, ws_gate, ws_up, ws_down)
    grads = pullback(grad_out)
    return (grads[0], grads[1], grads[2], grads[3], grads[4], grads[5], grads[6], grads[7])
```

```python
import functools
import jax
import jax.numpy as jnp
import numpy as np
from jax import lax
from jax.experimental import pallas as pl
from jax.experimental.pallas import tpu as pltpu
from jax.sharding import PartitionSpec as P

ALL_AXES = ("ep", "dp")
MESH = pl.DeviceIdType.MESH
LANE = 128
VMEM_LIMIT = 60 * 1024 * 1024
F32 = jnp.float32
BF16 = jnp.bfloat16


def pad_lanes(n):
    return (n + LANE - 1) // LANE * LANE


def dot(a, b):
    return lax.dot_general(a, b, (((1,), (0,)), ((), ())), preferred_element_type=F32)


def dot_rows(a, b):
    return lax.dot_general(a, b, (((0,), (0,)), ((), ())), preferred_element_type=F32)


def dot_cols(a, b):
    return lax.dot_general(a, b, (((1,), (1,)), ((), ())), preferred_element_type=F32)


def onehot(cond):
    return jnp.where(cond, 1.0, 0.0).astype(BF16)


def silu(x):
    return x * jax.nn.sigmoid(x)


def silu_grad(x):
    sigma = jax.nn.sigmoid(x)
    return sigma * (1.0 + x * (1.0 - sigma))


def roll_up(x, by):
    return pltpu.roll(x.astype(F32), by, 1)


def join(first, second):
    wide = first.shape[1]
    return jnp.concatenate([first[:, : wide - LANE], first[:, wide - LANE :] + second[:, :LANE], second[:, LANE:]], axis=1)


def spread(lo_ref, hi_ref, rows, at):
    width = rows.shape[1]
    wide = lo_ref.shape[1]
    count = rows.shape[0]
    lo_ref[at : at + count, :] = jnp.zeros((count, wide), BF16)
    lo_ref[at : at + count, :width] = rows
    hi_ref[at : at + count, :] = roll_up(lo_ref[at : at + count, :], wide - width).astype(BF16)


def fill_send(slot_rows, lo_ref, hi_ref, send_ref, per_copy):
    ep, cap, _ = send_ref.shape
    tokens = slot_rows.shape[1]
    step_size = 8
    row0 = slot_rows[0:1, :]
    row1 = slot_rows[1:2, :]

    def body(step, carry):
        shape = (step_size, cap, tokens)
        slot = (lax.broadcasted_iota(jnp.int32, shape, 0) + step * step_size) * (2 * cap) + lax.broadcasted_iota(jnp.int32, shape, 1)
        slot = slot.reshape(step_size * cap, tokens)

        def pick(s):
            if per_copy:
                return jnp.concatenate([onehot(row0 == s), onehot(row1 == s)], axis=1)
            return onehot((row0 == s) | (row1 == s))

        first = dot(pick(slot), lo_ref[...])
        second = dot(pick(slot + cap), hi_ref[...])
        send_ref[pl.ds(step * step_size, step_size)] = join(first, second).astype(BF16).reshape(step_size, cap, send_ref.shape[2])
        return carry

    lax.fori_loop(0, ep // step_size, body, 0)


def halves(ref, width, start=None, size=None):
    ep, cap, full = ref.shape
    wide = pad_lanes(width)
    block = ref[...] if start is None else ref[pl.ds(start, size)]
    block = block.reshape(block.shape[0] * cap, full)
    return block[:, :wide], block[:, full - wide :]


def collect(back_ref, slot_cols, slots_of_row, gate_cols, width, start, count):
    cap = back_ref.shape[1]
    first, second = halves(back_ref, width)
    cols = slot_cols[start : start + count, :]
    col0 = cols[:, 0:1]
    col1 = cols[:, 1:2]
    if gate_cols is None:
        acc0 = dot(onehot((col0 == slots_of_row) | (col1 == slots_of_row)), first)
        acc1 = dot(onehot((col0 == slots_of_row + cap) | (col1 == slots_of_row + cap)), second)
    else:
        gates = gate_cols[start : start + count, :]
        acc0 = gates[:, 0:1] * dot(onehot(col0 == slots_of_row), first) + gates[:, 1:2] * dot(onehot(col1 == slots_of_row), first)
        acc1 = gates[:, 0:1] * dot(onehot(col0 == slots_of_row + cap), second) + gates[:, 1:2] * dot(onehot(col1 == slots_of_row + cap), second)
    return (acc0 + roll_up(acc1, width))[:, :width]


def load_experts(gate_ref, up_ref, down_ref, w13_ref, w2_ref):
    width, ff = gate_ref.shape[1], gate_ref.shape[2]
    wide = w13_ref.shape[1]
    half = w13_ref.shape[2] // 2
    w13_ref[...] = jnp.zeros(w13_ref.shape, BF16)
    w2_ref[...] = jnp.zeros(w2_ref.shape, BF16)
    for e in range(2):
        at = e * (wide - width)
        w13_ref[e, at : at + width, :ff] = gate_ref[e]
        w13_ref[e, at : at + width, half : half + ff] = up_ref[e]
        w2_ref[e, :ff, :width] = down_ref[e]
    w2_ref[1] = roll_up(w2_ref[1], wide - width).astype(BF16)


STEP_DEV = 16


def experts_forward(recv_ref, w13_ref, w2_ref, send_ref, width):
    ep, cap, full = recv_ref.shape
    half = w13_ref.shape[2] // 2

    def body(step, carry):
        rows = halves(recv_ref, width, step * STEP_DEV, STEP_DEV)
        outs = []
        for e in range(2):
            pre = dot(rows[e], w13_ref[e])
            hidden = (silu(pre[:, :half]) * pre[:, half:]).astype(BF16)
            outs.append(dot(hidden, w2_ref[e]))
        send_ref[pl.ds(step * STEP_DEV, STEP_DEV)] = join(outs[0], outs[1]).astype(BF16).reshape(STEP_DEV, cap, full)
        return carry

    lax.fori_loop(0, ep // STEP_DEV, body, 0)


def experts_backward(recv_ref, grad_ref, w13_ref, w2_ref, send_ref, acc13_ref, acc2_ref, width):
    ep, cap, full = recv_ref.shape
    half = w13_ref.shape[2] // 2
    acc13_ref[...] = jnp.zeros(acc13_ref.shape, F32)
    acc2_ref[...] = jnp.zeros(acc2_ref.shape, F32)

    def body(step, carry):
        rows = halves(recv_ref, width, step * STEP_DEV, STEP_DEV)
        grads = halves(grad_ref, width, step * STEP_DEV, STEP_DEV)
        outs = []
        for e in range(2):
            pre = dot(rows[e], w13_ref[e])
            one, three = pre[:, :half], pre[:, half:]
            act = silu(one)
            hidden = (act * three).astype(BF16)
            grad_hidden = dot_cols(grads[e], w2_ref[e])
            grad_one = (grad_hidden * three * silu_grad(one)).astype(BF16)
            grad_three = (grad_hidden * act).astype(BF16)
            grad_pre = jnp.concatenate([grad_one, grad_three], axis=1)
            outs.append(dot_cols(grad_pre, w13_ref[e]))
            acc13_ref[e] += dot_rows(rows[e], grad_pre)
            acc2_ref[e] += dot_rows(hidden, grads[e])
        send_ref[pl.ds(step * STEP_DEV, STEP_DEV)] = join(outs[0], outs[1]).astype(BF16).reshape(STEP_DEV, cap, full)
        return carry

    lax.fori_loop(0, ep // STEP_DEV, body, 0)


def store_expert_grads(acc13_ref, acc2_ref, gate_out, up_out, down_out):
    width, ff = gate_out.shape[1], gate_out.shape[2]
    wide = acc13_ref.shape[1]
    half = acc13_ref.shape[2] // 2
    for e in range(2):
        at = e * (wide - width)
        gate_out[e] = acc13_ref[e, at : at + width, :ff].astype(BF16)
        up_out[e] = acc13_ref[e, at : at + width, half : half + ff].astype(BF16)
        down = acc2_ref[e]
        if e:
            down = roll_up(down, width)
        down_out[e] = down[:ff, :width].astype(BF16)


def dense_front(x, w_dense_ref):
    return (x.astype(F32) + dot(x, w_dense_ref[...])).astype(BF16)


def signal_peers(ep):
    barrier = pltpu.get_barrier_semaphore()
    me = lax.axis_index("ep")

    def body(i, carry):
        pl.semaphore_signal(barrier, inc=1, device_id={"ep": lax.rem(me + i, ep)}, device_id_type=MESH)
        return carry

    lax.fori_loop(1, ep, body, 0)


def wait_peers(ep):
    pl.semaphore_wait(pltpu.get_barrier_semaphore(), ep - 1)


def peer_of(i, ep):
    me = lax.axis_index("ep")
    turn = lax.rem(i - 1 + (ep // 2) * lax.axis_index("dp"), ep - 1) + 1
    return lax.rem(me + turn, ep)


def start_exchange(send_ref, recv_ref, send_sem, recv_sem, local_sem):
    ep = send_ref.shape[0]
    me = lax.axis_index("ep")

    def body(i, carry):
        peer = peer_of(i, ep)
        pltpu.make_async_remote_copy(
            src_ref=send_ref.at[peer],
            dst_ref=recv_ref.at[me],
            send_sem=send_sem.at[peer],
            recv_sem=recv_sem.at[me],
            device_id={"ep": peer},
            device_id_type=MESH,
        ).start()
        return carry

    lax.fori_loop(1, ep, body, 0)
    pltpu.make_async_copy(send_ref.at[me], recv_ref.at[me], local_sem).start()


def finish_exchange(send_ref, recv_ref, send_sem, recv_sem, local_sem):
    ep = send_ref.shape[0]
    me = lax.axis_index("ep")
    pltpu.make_async_copy(send_ref.at[me], recv_ref.at[me], local_sem).wait()

    def body(i, carry):
        peer = lax.rem(me + i, ep)
        copy = pltpu.make_async_remote_copy(
            src_ref=send_ref.at[peer],
            dst_ref=recv_ref.at[peer],
            send_sem=send_sem.at[peer],
            recv_sem=recv_sem.at[peer],
            device_id={"ep": peer},
            device_id_type=MESH,
        )
        copy.wait_send()
        copy.wait_recv()
        return carry

    lax.fori_loop(1, ep, body, 0)


def vmem():
    return pl.BlockSpec(memory_space=pltpu.VMEM)


def call(kernel, ins, outs, scratch, collective_id=None):
    return pl.pallas_call(
        kernel,
        out_shape=outs,
        in_specs=[vmem() for _ in ins],
        out_specs=tuple(vmem() for _ in outs),
        scratch_shapes=scratch,
        compiler_params=pltpu.CompilerParams(collective_id=collective_id, has_side_effects=collective_id is not None, vmem_limit_bytes=VMEM_LIMIT),
    )(*ins)


def exchange_scratch(ep):
    return [pltpu.SemaphoreType.DMA((ep,)), pltpu.SemaphoreType.DMA((ep,)), pltpu.SemaphoreType.DMA]


def shape(dims, dtype=BF16):
    return jax.ShapeDtypeStruct(dims, dtype)


def dispatch_kernel(x_ref, wd_ref, slot_row_ref, u_ref, recv_ref, send_ref, lo_ref, hi_ref, *sems):
    ep = recv_ref.shape[0]
    signal_peers(ep)
    u = dense_front(x_ref[...], wd_ref)
    u_ref[...] = u
    spread(lo_ref, hi_ref, u, 0)
    fill_send(slot_row_ref[...], lo_ref, hi_ref, send_ref, False)
    wait_peers(ep)
    start_exchange(send_ref, recv_ref, *sems)
    finish_exchange(send_ref, recv_ref, *sems)


def forward_kernel(rows_ref, gate_ref, up_ref, down_ref, recv_ref, send_ref, w13_ref, w2_ref, *sems):
    ep = recv_ref.shape[0]
    signal_peers(ep)
    load_experts(gate_ref, up_ref, down_ref, w13_ref, w2_ref)
    experts_forward(rows_ref, w13_ref, w2_ref, send_ref, gate_ref.shape[1])
    wait_peers(ep)
    start_exchange(send_ref, recv_ref, *sems)
    finish_exchange(send_ref, recv_ref, *sems)


def shared_out(u, s1_ref, s3_ref, s2_ref):
    one = dot(u, s1_ref[...])
    three = dot(u, s3_ref[...])
    return dot((silu(one) * three).astype(BF16), s2_ref[...])


def between_kernel(back_ref, slots_of_row_ref, slot_col_ref, gate_col_ref, u_ref, s1_ref, s3_ref, s2_ref, wd_ref, slot_row_ref, x_out_ref, u_out_ref, recv_ref, send_ref, lo_ref, hi_ref, *sems):
    ep = recv_ref.shape[0]
    tokens, width = u_ref.shape
    signal_peers(ep)
    count = 256
    for start in range(0, tokens, count):
        u = u_ref[start : start + count, :]
        routed = collect(back_ref, slot_col_ref, slots_of_row_ref[...], gate_col_ref, width, start, count)
        x = (u.astype(F32) + routed + shared_out(u, s1_ref, s3_ref, s2_ref)).astype(BF16)
        x_out_ref[start : start + count, :] = x
        mixed = dense_front(x, wd_ref)
        u_out_ref[start : start + count, :] = mixed
        spread(lo_ref, hi_ref, mixed, start)
    fill_send(slot_row_ref[...], lo_ref, hi_ref, send_ref, False)
    wait_peers(ep)
    start_exchange(send_ref, recv_ref, *sems)
    finish_exchange(send_ref, recv_ref, *sems)


def spread_gated(grad, gate_col_ref, lo_ref, hi_ref, start):
    tokens = gate_col_ref.shape[0]
    count = grad.shape[0]
    gates = gate_col_ref[start : start + count, :]
    for j in range(2):
        spread(lo_ref, hi_ref, (gates[:, j : j + 1] * grad.astype(F32)).astype(BF16), j * tokens + start)


def grad_dispatch_kernel(grad_ref, gate_col_ref, slot_row_ref, recv_ref, send_ref, lo_ref, hi_ref, *sems):
    ep = recv_ref.shape[0]
    signal_peers(ep)
    spread_gated(grad_ref[...], gate_col_ref, lo_ref, hi_ref, 0)
    fill_send(slot_row_ref[...], lo_ref, hi_ref, send_ref, True)
    wait_peers(ep)
    start_exchange(send_ref, recv_ref, *sems)
    finish_exchange(send_ref, recv_ref, *sems)


def backward_kernel(rows_ref, grads_ref, gate_ref, up_ref, down_ref, recv_ref, g_gate_ref, g_up_ref, g_down_ref, send_ref, w13_ref, w2_ref, acc13_ref, acc2_ref, *sems):
    ep = recv_ref.shape[0]
    signal_peers(ep)
    load_experts(gate_ref, up_ref, down_ref, w13_ref, w2_ref)
    experts_backward(rows_ref, grads_ref, w13_ref, w2_ref, send_ref, acc13_ref, acc2_ref, gate_ref.shape[1])
    wait_peers(ep)
    start_exchange(send_ref, recv_ref, *sems)
    store_expert_grads(acc13_ref, acc2_ref, g_gate_ref, g_up_ref, g_down_ref)
    finish_exchange(send_ref, recv_ref, *sems)


def shared_backward(grad, u, s1_ref, s3_ref, s2_ref, pack_ref, width, ff):
    one = dot(u, s1_ref[...])
    three = dot(u, s3_ref[...])
    act = silu(one)
    hidden = (act * three).astype(BF16)
    grad_hidden = dot_cols(grad, s2_ref[...])
    grad_one = (grad_hidden * three * silu_grad(one)).astype(BF16)
    grad_three = (grad_hidden * act).astype(BF16)
    at = pad_lanes(width)
    pack_ref[...] = jnp.zeros(pack_ref.shape, BF16)
    for part in (dot_rows(u, grad_one), dot_rows(u, grad_three), dot_rows(grad, hidden)):
        pack_ref[:, at : at + ff] = part.astype(BF16)
        at += pad_lanes(ff)
    return dot_cols(grad_one, s1_ref[...]) + dot_cols(grad_three, s3_ref[...])


def back_to_tokens(back_ref, slots_of_row_ref, slot_col_ref, grad_ref, u_ref, x_ref, s1_ref, s3_ref, s2_ref, wd_ref, pack_ref, mixed_ref, shared_ref, grad_x_ref):
    tokens, width = u_ref.shape
    ff = s1_ref.shape[1]
    shared_ref[...] = shared_backward(grad_ref[...], u_ref[...], s1_ref, s3_ref, s2_ref, pack_ref, width, ff)
    count = 256
    for start in range(0, tokens, count):
        rows = slice(start, start + count)
        routed = collect(back_ref, slot_col_ref, slots_of_row_ref[...], None, width, start, count)
        mixed = (grad_ref[rows, :].astype(F32) + routed + shared_ref[rows, :]).astype(BF16)
        mixed_ref[rows, :] = mixed
        grad_x_ref[rows, :] = (mixed.astype(F32) + dot_cols(mixed, wd_ref[...])).astype(BF16)
    pack_ref[:, :width] = dot_rows(x_ref[...], mixed_ref[...]).astype(BF16)


def turn_kernel(back_ref, slots_of_row_ref, slot_col_ref, grad_ref, u_ref, x_ref, s1_ref, s3_ref, s2_ref, wd_ref, gate_col_ref, slot_row_ref, grad_x_ref, pack_ref, recv_ref, send_ref, lo_ref, hi_ref, mixed_ref, shared_ref, *sems):
    ep = recv_ref.shape[0]
    signal_peers(ep)
    back_to_tokens(back_ref, slots_of_row_ref, slot_col_ref, grad_ref, u_ref, x_ref, s1_ref, s3_ref, s2_ref, wd_ref, pack_ref, mixed_ref, shared_ref, grad_x_ref)
    spread_gated(grad_x_ref[...], gate_col_ref, lo_ref, hi_ref, 0)
    fill_send(slot_row_ref[...], lo_ref, hi_ref, send_ref, True)
    wait_peers(ep)
    start_exchange(send_ref, recv_ref, *sems)
    finish_exchange(send_ref, recv_ref, *sems)


def last_kernel(back_ref, slots_of_row_ref, slot_col_ref, grad_ref, u_ref, x_ref, s1_ref, s3_ref, s2_ref, wd_ref, grad_x_ref, pack_ref, mixed_ref, shared_ref):
    back_to_tokens(back_ref, slots_of_row_ref, slot_col_ref, grad_ref, u_ref, x_ref, s1_ref, s3_ref, s2_ref, wd_ref, pack_ref, mixed_ref, shared_ref, grad_x_ref)


def remote(src, dst, send_sem, recv_sem, to):
    return pltpu.make_async_remote_copy(src_ref=src, dst_ref=dst, send_sem=send_sem, recv_sem=recv_sem, device_id=to, device_id_type=MESH)


TILE = 8


def sum_kernel(pack_ref, gate_ref, up_ref, down_ref, dense_out, gate_out, up_out, down_out, pair_ref, total_ref, parts_ref, mine_ref, full_ref, gate_in, up_in, down_in, pair_ssem, pair_rsem, rs_ssem, rs_rsem, ag_ssem, ag_rsem, local_sem):
    me = lax.axis_index("ep")
    core = lax.axis_index("dp")
    other = 1 - core
    ep = parts_ref.shape[0]
    owners = pack_ref.shape[1] // TILE
    barrier = pltpu.get_barrier_semaphore()
    signal_peers(ep)
    pl.semaphore_signal(barrier, inc=1, device_id={"dp": other}, device_id_type=MESH)
    pl.semaphore_wait(barrier, ep)
    partner = {"dp": other}
    pair = [
        remote(pack_ref.at[other], pair_ref, pair_ssem.at[0], pair_rsem.at[0], partner),
        remote(gate_ref, gate_in, pair_ssem.at[1], pair_rsem.at[1], partner),
        remote(up_ref, up_in, pair_ssem.at[2], pair_rsem.at[2], partner),
        remote(down_ref, down_in, pair_ssem.at[3], pair_rsem.at[3], partner),
    ]
    for copy in pair:
        copy.start()
    pair[0].wait_recv()
    summed = (pack_ref[core].astype(F32) + pair_ref[...].astype(F32)).astype(BF16)
    total_ref[...] = summed.reshape(total_ref.shape)

    def scatter(i, carry):
        peer = lax.rem(me + i, ep)

        @pl.when(peer < owners)
        def _():
            remote(total_ref.at[peer], parts_ref.at[me], rs_ssem.at[peer], rs_rsem.at[me], {"ep": peer}).start()

        return carry

    lax.fori_loop(1, ep, scatter, 0)

    def scatter_done(i, carry):
        peer = lax.rem(me + i, ep)

        @pl.when(peer < owners)
        def _():
            remote(total_ref.at[peer], parts_ref.at[me], rs_ssem.at[peer], rs_rsem.at[me], {"ep": peer}).wait_send()

        return carry

    @pl.when(me < owners)
    def _():
        parts_ref[me] = total_ref[me]

        def arrived(i, carry):
            peer = lax.rem(me + i, ep)
            remote(total_ref.at[0], parts_ref.at[peer], rs_ssem.at[peer], rs_rsem.at[peer], {"ep": peer}).wait_recv()
            return carry

        lax.fori_loop(1, ep, arrived, 0)
        mine_ref[...] = jnp.sum(parts_ref[...].astype(F32), axis=0).astype(BF16)

        def gather(i, carry):
            peer = lax.rem(me + i, ep)
            remote(mine_ref, full_ref.at[core, me], ag_ssem.at[peer], ag_rsem.at[me], {"ep": peer}).start()
            return carry

        lax.fori_loop(1, ep, gather, 0)
        full_ref[core, me] = mine_ref[...]

    lax.fori_loop(1, ep, scatter_done, 0)
    for copy, have, came, out in ((pair[1], gate_ref, gate_in, gate_out), (pair[2], up_ref, up_in, up_out), (pair[3], down_ref, down_in, down_out)):
        copy.wait_recv()
        out[...] = (have[...].astype(F32) + came[...].astype(F32)).astype(BF16)

    def gathered(i, carry):
        peer = lax.rem(me + i, ep)

        @pl.when(peer < owners)
        def _():
            remote(mine_ref, full_ref.at[core, peer], ag_ssem.at[peer], ag_rsem.at[peer], {"ep": peer}).wait_recv()

        return carry

    lax.fori_loop(1, ep, gathered, 0)
    swap = remote(full_ref.at[core], full_ref.at[core], pair_ssem.at[4], pair_rsem.at[4], partner)
    swap.start()

    @pl.when(me < owners)
    def _():
        def sent(i, carry):
            peer = lax.rem(me + i, ep)
            remote(mine_ref, full_ref.at[core, me], ag_ssem.at[peer], ag_rsem.at[me], {"ep": peer}).wait_send()
            return carry

        lax.fori_loop(1, ep, sent, 0)

    for copy in pair:
        copy.wait_send()
    swap.wait_send()
    remote(full_ref.at[other], full_ref.at[other], pair_ssem.at[4], pair_rsem.at[4], partner).wait_recv()
    dense_out[...] = full_ref[...].reshape(dense_out.shape)


def solution(mesh):
    ep = mesh.shape["ep"]
    tok_spec = P(ALL_AXES, None)
    route_spec = P(None, ALL_AXES, None)
    exp_spec = P(None, "ep", None, None)
    repl_spec = P(None, None, None)

    def body(act_in, grad_out, slot_ids, gate_vals, w_dense, w_gate, w_up, w_down, ws_gate, ws_up, ws_down):
        tokens, width = act_in.shape
        ff = w_gate.shape[3]
        local = w_gate.shape[1]
        cap = 2 * tokens * 2 // (local * ep)
        wide, half = pad_lanes(width), pad_lanes(ff)
        full = local * width
        block = (ep, cap, full)
        slot_rows = jnp.swapaxes(slot_ids, 1, 2)
        row = np.arange(ep * cap)
        slots_of_row = jnp.asarray(((row // cap) * local * cap + row % cap).astype(np.int32))[None, :]
        send = pltpu.VMEM(block, BF16)
        token_pads = [pltpu.VMEM((tokens, wide), BF16)] * 2
        copy_pads = [pltpu.VMEM((2 * tokens, wide), BF16)] * 2
        weights = [pltpu.VMEM((2, wide, 2 * half), BF16), pltpu.VMEM((2, half, wide), BF16)]
        accs = [pltpu.VMEM((2, wide, 2 * half), F32), pltpu.VMEM((2, half, wide), F32)]
        token_tmp = [pltpu.VMEM((tokens, width), BF16), pltpu.VMEM((tokens, width), F32)]
        sems = exchange_scratch(ep)
        tok = shape((tokens, width))
        pack_lanes = wide + 3 * half
        packed = shape((width, pack_lanes))
        eg = [shape((local, width, ff)), shape((local, width, ff)), shape((local, ff, width))]

        u1, rows1 = call(dispatch_kernel, (act_in, w_dense[0], slot_rows[0]), (tok, shape(block)), [send, *token_pads, *sems], 1)
        (grads2,) = call(grad_dispatch_kernel, (grad_out, gate_vals[1], slot_rows[1]), (shape(block),), [send, *copy_pads, *sems], 2)
        (back1,) = call(forward_kernel, (rows1, w_gate[0], w_up[0], w_down[0]), (shape(block),), [send, *weights, *sems], 3)
        x2, u2, rows2 = call(
            between_kernel,
            (back1, slots_of_row, slot_ids[0], gate_vals[0], u1, ws_gate[0], ws_up[0], ws_down[0], w_dense[1], slot_rows[1]),
            (tok, tok, shape(block)),
            [send, *token_pads, *sems],
            4,
        )
        back2, *eg2 = call(backward_kernel, (rows2, grads2, w_gate[1], w_up[1], w_down[1]), (shape(block), *eg), [send, *weights, *accs, *sems], 5)
        grad_x2, pack2, grads1 = call(
            turn_kernel,
            (back2, slots_of_row, slot_ids[1], grad_out, u2, x2, ws_gate[1], ws_up[1], ws_down[1], w_dense[1], gate_vals[0], slot_rows[0]),
            (tok, packed, shape(block)),
            [send, *copy_pads, *token_tmp, *sems],
            6,
        )
        back3, *eg1 = call(backward_kernel, (rows1, grads1, w_gate[0], w_up[0], w_down[0]), (shape(block), *eg), [send, *weights, *accs, *sems], 5)
        grad_act, pack1 = call(
            last_kernel,
            (back3, slots_of_row, slot_ids[0], grad_x2, u1, act_in, ws_gate[0], ws_up[0], ws_down[0], w_dense[0]),
            (tok, packed),
            token_tmp,
        )
        packs = jnp.stack([pack1, pack2])
        stacked = [jnp.stack([a, b]) for a, b in zip(eg1, eg2)]
        tiles = width // TILE
        es = [s.shape for s in stacked]
        sums, e_gate, e_up, e_down = call(
            sum_kernel,
            (packs, *stacked),
            (shape(packs.shape), *[shape(s) for s in es]),
            [
                pltpu.VMEM((width, pack_lanes), BF16),
                pltpu.VMEM((tiles, TILE, pack_lanes), BF16),
                pltpu.VMEM((ep, TILE, pack_lanes), BF16),
                pltpu.VMEM((TILE, pack_lanes), BF16),
                pltpu.VMEM((2, tiles, TILE, pack_lanes), BF16),
                *[pltpu.VMEM(s, BF16) for s in es],
                pltpu.SemaphoreType.DMA((5,)),
                pltpu.SemaphoreType.DMA((5,)),
                pltpu.SemaphoreType.DMA((ep,)),
                pltpu.SemaphoreType.DMA((ep,)),
                pltpu.SemaphoreType.DMA((ep,)),
                pltpu.SemaphoreType.DMA((ep,)),
                pltpu.SemaphoreType.DMA,
            ],
            7,
        )
        g_dense = sums[:, :, :width]
        g_s1 = sums[:, :, wide : wide + ff]
        g_s3 = sums[:, :, wide + half : wide + half + ff]
        g_s2 = jnp.swapaxes(sums[:, :, wide + 2 * half : wide + 2 * half + ff], 1, 2)
        return (grad_act, g_dense, e_gate, e_up, e_down, g_s1, g_s3, g_s2)

    return jax.shard_map(body, mesh=mesh, in_specs=(tok_spec, tok_spec, route_spec, route_spec, repl_spec, exp_spec, exp_spec, exp_spec, repl_spec, repl_spec, repl_spec), out_specs=(tok_spec, repl_spec, exp_spec, exp_spec, exp_spec, repl_spec, repl_spec, repl_spec), check_vma=False)
```

```python
import functools
import jax
import jax.numpy as jnp
import numpy as np
from jax import lax
from jax.experimental import pallas as pl
from jax.experimental.pallas import tpu as pltpu
from jax.sharding import PartitionSpec as P

ALL_AXES = ("ep", "dp")
MESH = pl.DeviceIdType.MESH
LANE = 128
VMEM_LIMIT = 60 * 1024 * 1024
F32 = jnp.float32
BF16 = jnp.bfloat16


def pad_lanes(n):
    return (n + LANE - 1) // LANE * LANE


def dot(a, b):
    return lax.dot_general(a, b, (((1,), (0,)), ((), ())), preferred_element_type=F32)


def dot_rows(a, b):
    return lax.dot_general(a, b, (((0,), (0,)), ((), ())), preferred_element_type=F32)


def dot_cols(a, b):
    return lax.dot_general(a, b, (((1,), (1,)), ((), ())), preferred_element_type=F32)


def onehot(cond):
    return jnp.where(cond, 1.0, 0.0).astype(BF16)


def silu(x):
    return x * jax.nn.sigmoid(x)


def silu_grad(x):
    sigma = jax.nn.sigmoid(x)
    return sigma * (1.0 + x * (1.0 - sigma))


def roll_up(x, by):
    return pltpu.roll(x.astype(F32), by, 1)


def join(first, second):
    wide = first.shape[1]
    return jnp.concatenate([first[:, : wide - LANE], first[:, wide - LANE :] + second[:, :LANE], second[:, LANE:]], axis=1)


def spread(lo_ref, hi_ref, rows, at):
    width = rows.shape[1]
    wide = lo_ref.shape[1]
    count = rows.shape[0]
    lo_ref[at : at + count, :] = jnp.zeros((count, wide), BF16)
    lo_ref[at : at + count, :width] = rows
    hi_ref[at : at + count, :] = roll_up(lo_ref[at : at + count, :], wide - width).astype(BF16)


CHUNK = 8
GROUP = 32


def fill_send(slot_rows, lo_ref, hi_ref, send_ref, chunk, per_copy):
    ep, cap, _ = send_ref.shape
    tokens = slot_rows.shape[1]
    row0 = slot_rows[0:1, :]
    row1 = slot_rows[1:2, :]
    rows = pl.ds(chunk * CHUNK, CHUNK)

    def body(step, carry):
        dims = (GROUP, CHUNK, tokens)
        slot = (lax.broadcasted_iota(jnp.int32, dims, 0) + step * GROUP) * (2 * cap) + lax.broadcasted_iota(jnp.int32, dims, 1)
        slot = slot.reshape(GROUP * CHUNK, tokens) + chunk * CHUNK

        def pick(s):
            if per_copy:
                return jnp.concatenate([onehot(row0 == s), onehot(row1 == s)], axis=1)
            return onehot((row0 == s) | (row1 == s))

        first = dot(pick(slot), lo_ref[...])
        second = dot(pick(slot + cap), hi_ref[...])
        send_ref[pl.ds(step * GROUP, GROUP), rows] = join(first, second).astype(BF16).reshape(GROUP, CHUNK, send_ref.shape[2])
        return carry

    lax.fori_loop(0, ep // GROUP, body, 0)


def halves(ref, width, step=None, chunk=None):
    full = ref.shape[2]
    wide = pad_lanes(width)
    block = ref[...] if step is None else ref[pl.ds(step * GROUP, GROUP), pl.ds(chunk * CHUNK, CHUNK)]
    block = block.reshape(block.shape[0] * block.shape[1], full)
    return block[:, :wide], block[:, full - wide :]


def collect(back_ref, slot_cols, slots_of_row, gate_cols, width, start, count):
    cap = back_ref.shape[1]
    first, second = halves(back_ref, width)
    cols = slot_cols[start : start + count, :]
    col0 = cols[:, 0:1]
    col1 = cols[:, 1:2]
    if gate_cols is None:
        acc0 = dot(onehot((col0 == slots_of_row) | (col1 == slots_of_row)), first)
        acc1 = dot(onehot((col0 == slots_of_row + cap) | (col1 == slots_of_row + cap)), second)
    else:
        gates = gate_cols[start : start + count, :]
        acc0 = gates[:, 0:1] * dot(onehot(col0 == slots_of_row), first) + gates[:, 1:2] * dot(onehot(col1 == slots_of_row), first)
        acc1 = gates[:, 0:1] * dot(onehot(col0 == slots_of_row + cap), second) + gates[:, 1:2] * dot(onehot(col1 == slots_of_row + cap), second)
    return (acc0 + roll_up(acc1, width))[:, :width]


def load_experts(gate_ref, up_ref, down_ref, w13_ref, w2_ref):
    width, ff = gate_ref.shape[1], gate_ref.shape[2]
    wide = w13_ref.shape[1]
    half = w13_ref.shape[2] // 2
    w13_ref[...] = jnp.zeros(w13_ref.shape, BF16)
    w2_ref[...] = jnp.zeros(w2_ref.shape, BF16)
    for e in range(2):
        at = e * (wide - width)
        w13_ref[e, at : at + width, :ff] = gate_ref[e]
        w13_ref[e, at : at + width, half : half + ff] = up_ref[e]
        w2_ref[e, :ff, :width] = down_ref[e]
    w2_ref[1] = roll_up(w2_ref[1], wide - width).astype(BF16)


def experts_forward(recv_ref, w13_ref, w2_ref, send_ref, width, chunk):
    ep, cap, full = recv_ref.shape
    half = w13_ref.shape[2] // 2

    def body(step, carry):
        rows = halves(recv_ref, width, step, chunk)
        outs = []
        for e in range(2):
            pre = dot(rows[e], w13_ref[e])
            hidden = (silu(pre[:, :half]) * pre[:, half:]).astype(BF16)
            outs.append(dot(hidden, w2_ref[e]))
        send_ref[pl.ds(step * GROUP, GROUP), pl.ds(chunk * CHUNK, CHUNK)] = join(outs[0], outs[1]).astype(BF16).reshape(GROUP, CHUNK, full)
        return carry

    lax.fori_loop(0, ep // GROUP, body, 0)


def experts_backward(recv_ref, grad_ref, w13_ref, w2_ref, send_ref, acc13_ref, acc2_ref, width, chunk):
    ep, cap, full = recv_ref.shape
    half = w13_ref.shape[2] // 2
    if chunk == 0:
        acc13_ref[...] = jnp.zeros(acc13_ref.shape, F32)
        acc2_ref[...] = jnp.zeros(acc2_ref.shape, F32)

    def body(step, carry):
        rows = halves(recv_ref, width, step, chunk)
        grads = halves(grad_ref, width, step, chunk)
        outs = []
        for e in range(2):
            pre = dot(rows[e], w13_ref[e])
            one, three = pre[:, :half], pre[:, half:]
            act = silu(one)
            hidden = (act * three).astype(BF16)
            grad_hidden = dot_cols(grads[e], w2_ref[e])
            grad_one = (grad_hidden * three * silu_grad(one)).astype(BF16)
            grad_three = (grad_hidden * act).astype(BF16)
            grad_pre = jnp.concatenate([grad_one, grad_three], axis=1)
            outs.append(dot_cols(grad_pre, w13_ref[e]))
            acc13_ref[e] += dot_rows(rows[e], grad_pre)
            acc2_ref[e] += dot_rows(hidden, grads[e])
        send_ref[pl.ds(step * GROUP, GROUP), pl.ds(chunk * CHUNK, CHUNK)] = join(outs[0], outs[1]).astype(BF16).reshape(GROUP, CHUNK, full)
        return carry

    lax.fori_loop(0, ep // GROUP, body, 0)


def store_expert_grads(acc13_ref, acc2_ref, gate_out, up_out, down_out):
    width, ff = gate_out.shape[1], gate_out.shape[2]
    wide = acc13_ref.shape[1]
    half = acc13_ref.shape[2] // 2
    for e in range(2):
        at = e * (wide - width)
        gate_out[e] = acc13_ref[e, at : at + width, :ff].astype(BF16)
        up_out[e] = acc13_ref[e, at : at + width, half : half + ff].astype(BF16)
        down = acc2_ref[e]
        if e:
            down = roll_up(down, width)
        down_out[e] = down[:ff, :width].astype(BF16)


def dense_front(x, w_dense_ref):
    return (x.astype(F32) + dot(x, w_dense_ref[...])).astype(BF16)


def signal_peers(ep):
    barrier = pltpu.get_barrier_semaphore()
    me = lax.axis_index("ep")

    def body(i, carry):
        pl.semaphore_signal(barrier, inc=1, device_id={"ep": lax.rem(me + i, ep)}, device_id_type=MESH)
        return carry

    lax.fori_loop(1, ep, body, 0)


def wait_peers(ep):
    pl.semaphore_wait(pltpu.get_barrier_semaphore(), ep - 1)


def peer_of(i, ep):
    me = lax.axis_index("ep")
    turn = lax.rem(i - 1 + (ep // 2) * lax.axis_index("dp"), ep - 1) + 1
    return lax.rem(me + turn, ep)


def remote(src, dst, send_sem, recv_sem, to):
    return pltpu.make_async_remote_copy(src_ref=src, dst_ref=dst, send_sem=send_sem, recv_sem=recv_sem, device_id=to, device_id_type=MESH)


class Exchange:
    def __init__(self, send, recv, send_sem, recv_sem, local_sem):
        self.send, self.recv, self.send_sem, self.recv_sem, self.local_sem = send, recv, send_sem, recv_sem, local_sem
        self.ep, cap, _ = send.shape
        self.chunks = cap // CHUNK
        self.me = lax.axis_index("ep")

    def copy(self, chunk, peer, to):
        rows = pl.ds(chunk * CHUNK, CHUNK)
        return remote(self.send.at[peer, rows], self.recv.at[to, rows], self.send_sem.at[chunk, peer], self.recv_sem.at[chunk, to], {"ep": peer})

    def own(self, chunk):
        rows = pl.ds(chunk * CHUNK, CHUNK)
        return pltpu.make_async_copy(self.send.at[self.me, rows], self.recv.at[self.me, rows], self.local_sem.at[chunk])

    def start(self, chunk):
        def body(i, carry):
            self.copy(chunk, peer_of(i, self.ep), self.me).start()
            return carry

        lax.fori_loop(1, self.ep, body, 0)
        self.own(chunk).start()

    def wait_recv(self, chunk):
        self.own(chunk).wait()

        def body(i, carry):
            peer = lax.rem(self.me + i, self.ep)
            self.copy(chunk, peer, peer).wait_recv()
            return carry

        lax.fori_loop(1, self.ep, body, 0)

    def wait_send(self):
        for chunk in range(self.chunks):

            def body(i, carry):
                self.copy(chunk, lax.rem(self.me + i, self.ep), self.me).wait_send()
                return carry

            lax.fori_loop(1, self.ep, body, 0)


def vmem():
    return pl.BlockSpec(memory_space=pltpu.VMEM)


def call(kernel, ins, outs, scratch, collective_id=None):
    return pl.pallas_call(
        kernel,
        out_shape=outs,
        in_specs=[vmem() for _ in ins],
        out_specs=tuple(vmem() for _ in outs),
        scratch_shapes=scratch,
        compiler_params=pltpu.CompilerParams(collective_id=collective_id, has_side_effects=collective_id is not None, vmem_limit_bytes=VMEM_LIMIT),
    )(*ins)


def exchange_scratch(ep, cap):
    return [pltpu.SemaphoreType.DMA((cap // CHUNK, ep)), pltpu.SemaphoreType.DMA((cap // CHUNK, ep)), pltpu.SemaphoreType.DMA((cap // CHUNK,))]


def shape(dims, dtype=BF16):
    return jax.ShapeDtypeStruct(dims, dtype)


def shared_out(u, s1_ref, s3_ref, s2_ref):
    one = dot(u, s1_ref[...])
    three = dot(u, s3_ref[...])
    return dot((silu(one) * three).astype(BF16), s2_ref[...])


def spread_gated(grad, gate_col_ref, lo_ref, hi_ref, start):
    tokens = gate_col_ref.shape[0]
    count = grad.shape[0]
    gates = gate_col_ref[start : start + count, :]
    for j in range(2):
        spread(lo_ref, hi_ref, (gates[:, j : j + 1] * grad.astype(F32)).astype(BF16), j * tokens + start)


def first_kernel(x_ref, wd_ref, slot_row_ref, gate_ref, up_ref, down_ref, grad_ref, gate_col_ref, grad_slot_row_ref, u_ref, rows_ref, grads_ref, back_ref, send_ref, lo_ref, hi_ref, grad_send_ref, grad_lo_ref, grad_hi_ref, back_send_ref, w13_ref, w2_ref, *sems):
    ep = rows_ref.shape[0]
    width = x_ref.shape[1]
    signal_peers(ep)
    out = Exchange(send_ref, rows_ref, *sems[0:3])
    grads = Exchange(grad_send_ref, grads_ref, *sems[3:6])
    back = Exchange(back_send_ref, back_ref, *sems[6:9])
    u = dense_front(x_ref[...], wd_ref)
    u_ref[...] = u
    spread(lo_ref, hi_ref, u, 0)
    for chunk in range(out.chunks):
        fill_send(slot_row_ref[...], lo_ref, hi_ref, send_ref, chunk, False)
        if chunk == 0:
            wait_peers(ep)
        out.start(chunk)
    load_experts(gate_ref, up_ref, down_ref, w13_ref, w2_ref)
    spread_gated(grad_ref[...], gate_col_ref, grad_lo_ref, grad_hi_ref, 0)
    for chunk in range(out.chunks):
        fill_send(grad_slot_row_ref[...], grad_lo_ref, grad_hi_ref, grad_send_ref, chunk, True)
    for chunk in range(out.chunks):
        out.wait_recv(chunk)
        experts_forward(rows_ref, w13_ref, w2_ref, back_send_ref, width, chunk)
        back.start(chunk)
        grads.start(chunk)
    for chunk in range(out.chunks):
        grads.wait_recv(chunk)
        back.wait_recv(chunk)
    for e in (out, grads, back):
        e.wait_send()


def middle_kernel(back_ref, slots_of_row_ref, slot_col_ref, gate_col_ref, u1_ref, s1_ref, s3_ref, s2_ref, wd_ref, slot_row_ref, grads_ref, gate_ref, up_ref, down_ref, x_ref, u_ref, ret_ref, g_gate_ref, g_up_ref, g_down_ref, rows_ref, send_ref, lo_ref, hi_ref, ret_send_ref, w13_ref, w2_ref, acc13_ref, acc2_ref, *sems):
    ep = rows_ref.shape[0]
    tokens, width = u1_ref.shape
    signal_peers(ep)
    out = Exchange(send_ref, rows_ref, *sems[0:3])
    ret = Exchange(ret_send_ref, ret_ref, *sems[3:6])
    count = 256
    for start in range(0, tokens, count):
        u = u1_ref[start : start + count, :]
        routed = collect(back_ref, slot_col_ref, slots_of_row_ref[...], gate_col_ref, width, start, count)
        x = (u.astype(F32) + routed + shared_out(u, s1_ref, s3_ref, s2_ref)).astype(BF16)
        x_ref[start : start + count, :] = x
        mixed = dense_front(x, wd_ref)
        u_ref[start : start + count, :] = mixed
        spread(lo_ref, hi_ref, mixed, start)
    for chunk in range(out.chunks):
        fill_send(slot_row_ref[...], lo_ref, hi_ref, send_ref, chunk, False)
        if chunk == 0:
            wait_peers(ep)
        out.start(chunk)
    load_experts(gate_ref, up_ref, down_ref, w13_ref, w2_ref)
    for chunk in range(out.chunks):
        out.wait_recv(chunk)
        experts_backward(rows_ref, grads_ref, w13_ref, w2_ref, ret_send_ref, acc13_ref, acc2_ref, width, chunk)
        ret.start(chunk)
    store_expert_grads(acc13_ref, acc2_ref, g_gate_ref, g_up_ref, g_down_ref)
    for chunk in range(out.chunks):
        ret.wait_recv(chunk)
    for e in (out, ret):
        e.wait_send()


def shared_back(grad, u, s1_ref, s3_ref, s2_ref, hid_ref, one_ref, three_ref):
    one = dot(u, s1_ref[...])
    three = dot(u, s3_ref[...])
    act = silu(one)
    hid_ref[...] = (act * three).astype(BF16)
    grad_hidden = dot_cols(grad, s2_ref[...])
    one_ref[...] = (grad_hidden * three * silu_grad(one)).astype(BF16)
    three_ref[...] = (grad_hidden * act).astype(BF16)
    return dot_cols(one_ref[...], s1_ref[...]) + dot_cols(three_ref[...], s3_ref[...])


TILE = 8


class DenseSum:
    def __init__(self, pack, full, pair, total, parts, mine, pair_ssem, pair_rsem, rs_ssem, rs_rsem, ag_ssem, ag_rsem):
        self.pack, self.full, self.pair, self.total, self.parts, self.mine = pack, full, pair, total, parts, mine
        self.pair_ssem, self.pair_rsem = pair_ssem, pair_rsem
        self.rs_ssem, self.rs_rsem, self.ag_ssem, self.ag_rsem = rs_ssem, rs_rsem, ag_ssem, ag_rsem
        self.me = lax.axis_index("ep")
        self.core = lax.axis_index("dp")
        self.ep = parts.shape[0]
        self.owners = total.shape[0]

    def each(self, act, owners=False):
        def body(i, carry):
            peer = lax.rem(self.me + i, self.ep)
            if owners:
                pl.when(peer < self.owners)(lambda: act(peer))
            else:
                act(peer)
            return carry

        lax.fori_loop(1, self.ep, body, 0)

    def pair_copy(self):
        return remote(self.pack.at[1 - self.core], self.pair, self.pair_ssem.at[0], self.pair_rsem.at[0], {"dp": 1 - self.core})

    def scatter_copy(self, peer, tile, to):
        return remote(self.total.at[tile], self.parts.at[to], self.rs_ssem.at[peer], self.rs_rsem.at[to], {"ep": peer})

    def gather_copy(self, peer, to):
        return remote(self.mine, self.full.at[self.core, to], self.ag_ssem.at[peer], self.ag_rsem.at[to], {"ep": peer})

    def swap_copy(self, half):
        return remote(self.full.at[half], self.full.at[half], self.pair_ssem.at[1], self.pair_rsem.at[1], {"dp": 1 - self.core})

    def start_pair(self):
        self.pair_copy().start()

    def scatter(self):
        self.pair_copy().wait_recv()
        both = (self.pack[self.core].astype(F32) + self.pair[...].astype(F32)).astype(BF16)
        self.total[...] = both.reshape(self.total.shape)
        self.each(lambda peer: self.scatter_copy(peer, peer, self.me).start(), owners=True)

    def gather(self):
        @pl.when(self.me < self.owners)
        def _():
            self.parts[self.me] = self.total[self.me]
            self.each(lambda peer: self.scatter_copy(peer, 0, peer).wait_recv())
            self.mine[...] = jnp.sum(self.parts[...].astype(F32), axis=0).astype(BF16)
            self.each(lambda peer: self.gather_copy(peer, self.me).start())
            self.full[self.core, self.me] = self.mine[...]

        self.each(lambda peer: self.scatter_copy(peer, peer, self.me).wait_send(), owners=True)

    def swap(self):
        self.each(lambda peer: self.gather_copy(peer, peer).wait_recv(), owners=True)
        self.swap_copy(self.core).start()

        @pl.when(self.me < self.owners)
        def _():
            self.each(lambda peer: self.gather_copy(peer, self.me).wait_send())

    def finish(self):
        self.pair_copy().wait_send()
        self.swap_copy(self.core).wait_send()
        self.swap_copy(1 - self.core).wait_recv()


def sum_scratch(ep, rows, lanes):
    tiles = rows // TILE
    return [
        pltpu.VMEM((rows, lanes), BF16),
        pltpu.VMEM((tiles, TILE, lanes), BF16),
        pltpu.VMEM((ep, TILE, lanes), BF16),
        pltpu.VMEM((TILE, lanes), BF16),
        pltpu.SemaphoreType.DMA((2,)),
        pltpu.SemaphoreType.DMA((2,)),
        *[pltpu.SemaphoreType.DMA((ep,))] * 4,
    ]


def signal_partner():
    pl.semaphore_signal(pltpu.get_barrier_semaphore(), inc=1, device_id={"dp": 1 - lax.axis_index("dp")}, device_id_type=MESH)


def wait_everyone(ep):
    pl.semaphore_wait(pltpu.get_barrier_semaphore(), ep)


def turn_kernel(ret2_ref, slots_of_row_ref, slot_col_ref, grad_ref, u2_ref, x2_ref, s1_ref, s3_ref, s2_ref, wd_ref, gate_col_ref, slot_row_ref, rows_ref, gate_ref, up_ref, down_ref, u1_ref, s1a_ref, s3a_ref, s2a_ref, grad_x_ref, shared_ref, ret_ref, g_gate_ref, g_up_ref, g_down_ref, full_ref, grads_ref, send_ref, lo_ref, hi_ref, ret_send_ref, w13_ref, w2_ref, acc13_ref, acc2_ref, mixed_ref, hid_ref, one_ref, three_ref, pack_ref, *rest):
    ep = rows_ref.shape[0]
    tokens, width = u2_ref.shape
    ff = s1_ref.shape[1]
    wide, half = pad_lanes(width), pad_lanes(ff)
    signal_peers(ep)
    signal_partner()
    out = Exchange(send_ref, grads_ref, *rest[0:3])
    ret = Exchange(ret_send_ref, ret_ref, *rest[3:6])
    dense = DenseSum(pack_ref, full_ref, *rest[6:16])
    shared_ref[...] = shared_back(grad_ref[...], u2_ref[...], s1_ref, s3_ref, s2_ref, hid_ref, one_ref, three_ref)
    count = 256
    for start in range(0, tokens, count):
        rows = slice(start, start + count)
        routed = collect(ret2_ref, slot_col_ref, slots_of_row_ref[...], None, width, start, count)
        mixed = (grad_ref[rows, :].astype(F32) + routed + shared_ref[rows, :]).astype(BF16)
        mixed_ref[rows, :] = mixed
        grad_x = (mixed.astype(F32) + dot_cols(mixed, wd_ref[...])).astype(BF16)
        grad_x_ref[rows, :] = grad_x
        spread_gated(grad_x, gate_col_ref, lo_ref, hi_ref, start)
    for chunk in range(out.chunks):
        fill_send(slot_row_ref[...], lo_ref, hi_ref, send_ref, chunk, True)
        if chunk == 0:
            wait_everyone(ep)
        out.start(chunk)
    load_experts(gate_ref, up_ref, down_ref, w13_ref, w2_ref)
    pack_ref[...] = jnp.zeros(pack_ref.shape, BF16)
    pack_ref[0, :, :width] = dot_rows(x2_ref[...], mixed_ref[...]).astype(BF16)
    pack_ref[0, :, wide : wide + ff] = dot_rows(u2_ref[...], one_ref[...]).astype(BF16)
    pack_ref[1, :, :ff] = dot_rows(u2_ref[...], three_ref[...]).astype(BF16)
    pack_ref[1, :, half : half + ff] = dot_rows(grad_ref[...], hid_ref[...]).astype(BF16)
    shared_ref[...] = shared_back(grad_x_ref[...], u1_ref[...], s1a_ref, s3a_ref, s2a_ref, hid_ref, one_ref, three_ref)
    pack_ref[0, :, wide + half : wide + half + ff] = dot_rows(u1_ref[...], one_ref[...]).astype(BF16)
    pack_ref[1, :, 2 * half : 2 * half + ff] = dot_rows(u1_ref[...], three_ref[...]).astype(BF16)
    pack_ref[1, :, 3 * half : 3 * half + ff] = dot_rows(grad_x_ref[...], hid_ref[...]).astype(BF16)
    dense.start_pair()
    for chunk in range(out.chunks):
        out.wait_recv(chunk)
        experts_backward(rows_ref, grads_ref, w13_ref, w2_ref, ret_send_ref, acc13_ref, acc2_ref, width, chunk)
        ret.start(chunk)
        if chunk == 0:
            dense.scatter()
    store_expert_grads(acc13_ref, acc2_ref, g_gate_ref, g_up_ref, g_down_ref)
    dense.gather()
    for chunk in range(out.chunks):
        ret.wait_recv(chunk)
    dense.swap()
    for e in (out, ret):
        e.wait_send()
    dense.finish()


def last_kernel(ret_ref, slots_of_row_ref, slot_col_ref, grad_ref, shared_ref, x_ref, wd_ref, sums_ref, gate1_ref, up1_ref, down1_ref, gate2_ref, up2_ref, down2_ref, grad_x_ref, dense_out, gate_out, up_out, down_out, s1_out, s3_out, s2_out, mixed_ref, pack_ref, full_ref, gate_in, up_in, down_in, e_ssem, e_rsem, *sums):
    tokens, width = x_ref.shape
    ff = s1_out.shape[2]
    wide, half = pad_lanes(width), pad_lanes(ff)
    dense = DenseSum(pack_ref, full_ref, *sums)
    signal_peers(dense.ep)
    signal_partner()
    other = {"dp": 1 - dense.core}
    mine = ((gate1_ref, gate2_ref, gate_in, gate_out), (up1_ref, up2_ref, up_in, up_out), (down1_ref, down2_ref, down_in, down_out))
    pairs = [(remote(refs[k], refs[2].at[k], e_ssem.at[n, k], e_rsem.at[n, k], other)) for n, refs in enumerate(mine) for k in range(2)]
    wait_everyone(dense.ep)
    for copy in pairs:
        copy.start()
    count = 256
    for start in range(0, tokens, count):
        rows = slice(start, start + count)
        routed = collect(ret_ref, slot_col_ref, slots_of_row_ref[...], None, width, start, count)
        mixed_ref[rows, :] = (grad_ref[rows, :].astype(F32) + routed + shared_ref[rows, :]).astype(BF16)
    part = dot_rows(x_ref[...], mixed_ref[...]).astype(BF16)
    lanes = pack_ref.shape[2]
    pack_ref[...] = jnp.zeros(pack_ref.shape, BF16)
    pack_ref[0] = part[:, :lanes]
    pack_ref[1, :, : width - lanes] = part[:, lanes:]
    dense.start_pair()
    dense.scatter()
    grad_x_ref[...] = (mixed_ref[...].astype(F32) + dot_cols(mixed_ref[...], wd_ref[...])).astype(BF16)
    for n, refs in enumerate(mine):
        for k in range(2):
            pairs[2 * n + k].wait_recv()
            refs[3][k] = (refs[k][...].astype(F32) + refs[2][k].astype(F32)).astype(BF16)
    dense.gather()
    dense_out[1] = sums_ref[0, :, :width]
    for k, (at1, at3) in enumerate(((wide + half, 2 * half), (wide, 0))):
        s1_out[k] = sums_ref[0, :, at1 : at1 + ff]
        s3_out[k] = sums_ref[1, :, at3 : at3 + ff]
        down = sums_ref[1, :, at3 + half : at3 + 2 * half].astype(F32)
        s2_out[k] = jnp.transpose(down)[:ff, :].astype(BF16)
    dense.swap()
    for copy in pairs:
        copy.wait_send()
    dense.finish()
    dense_out[0, :, :lanes] = full_ref[0].reshape(width, lanes)
    dense_out[0, :, lanes:] = full_ref[1].reshape(width, lanes)[:, : width - lanes]


def solution(mesh):
    ep = mesh.shape["ep"]
    tok_spec = P(ALL_AXES, None)
    route_spec = P(None, ALL_AXES, None)
    exp_spec = P(None, "ep", None, None)
    repl_spec = P(None, None, None)

    def body(act_in, grad_out, slot_ids, gate_vals, w_dense, w_gate, w_up, w_down, ws_gate, ws_up, ws_down):
        tokens, width = act_in.shape
        ff = w_gate.shape[3]
        local = w_gate.shape[1]
        cap = 2 * tokens * 2 // (local * ep)
        wide, half = pad_lanes(width), pad_lanes(ff)
        block = (ep, cap, local * width)
        slot_rows = jnp.swapaxes(slot_ids, 1, 2)
        row = np.arange(ep * cap)
        slots_of_row = jnp.asarray(((row // cap) * local * cap + row % cap).astype(np.int32))[None, :]
        send = pltpu.VMEM(block, BF16)
        token_pads = [pltpu.VMEM((tokens, wide), BF16)] * 2
        copy_pads = [pltpu.VMEM((2 * tokens, wide), BF16)] * 2
        weights = [pltpu.VMEM((2, wide, 2 * half), BF16), pltpu.VMEM((2, half, wide), BF16)]
        accs = [pltpu.VMEM((2, wide, 2 * half), F32), pltpu.VMEM((2, half, wide), F32)]
        hidden_tmp = [pltpu.VMEM((tokens, ff), BF16)] * 3
        sems = exchange_scratch(ep, cap)
        tok = shape((tokens, width))
        blk = shape(block)
        eg = [shape((local, width, ff)), shape((local, width, ff)), shape((local, ff, width))]
        lanes = wide + 2 * half + 2 * LANE
        tiles = width // TILE

        u1, rows1, grads2, back1 = call(
            first_kernel,
            (act_in, w_dense[0], slot_rows[0], w_gate[0], w_up[0], w_down[0], grad_out, gate_vals[1], slot_rows[1]),
            (tok, blk, blk, blk),
            [send, *token_pads, send, *copy_pads, send, *weights, *sems, *sems, *sems],
            1,
        )
        x2, u2, ret2, *eg2 = call(
            middle_kernel,
            (back1, slots_of_row, slot_ids[0], gate_vals[0], u1, ws_gate[0], ws_up[0], ws_down[0], w_dense[1], slot_rows[1], grads2, w_gate[1], w_up[1], w_down[1]),
            (tok, tok, blk, *eg),
            [send, send, *token_pads, send, *weights, *accs, *sems, *sems],
            2,
        )
        grad_x2, shared1, ret1, eg_gate, eg_up, eg_down, sums = call(
            turn_kernel,
            (ret2, slots_of_row, slot_ids[1], grad_out, u2, x2, ws_gate[1], ws_up[1], ws_down[1], w_dense[1], gate_vals[0], slot_rows[0], rows1, w_gate[0], w_up[0], w_down[0], u1, ws_gate[0], ws_up[0], ws_down[0]),
            (tok, shape((tokens, width), F32), blk, *eg, shape((2, tiles, TILE, lanes))),
            [send, send, *copy_pads, send, *weights, *accs, pltpu.VMEM((tokens, width), BF16), *hidden_tmp, pltpu.VMEM((2, width, lanes), BF16), *sems, *sems, *sum_scratch(ep, width, lanes)],
            3,
        )
        last_lanes = wide // 2
        pairs = [(2, local, width, ff), (2, local, width, ff), (2, local, ff, width)]
        return call(
            last_kernel,
            (ret1, slots_of_row, slot_ids[0], grad_x2, shared1, act_in, w_dense[0], sums.reshape(2, width, lanes), eg_gate, eg_up, eg_down, *eg2),
            (tok, shape((2, width, width)), *[shape(s) for s in pairs], shape((2, width, ff)), shape((2, width, ff)), shape((2, ff, width))),
            [
                pltpu.VMEM((tokens, width), BF16),
                pltpu.VMEM((2, width, last_lanes), BF16),
                pltpu.VMEM((2, tiles, TILE, last_lanes), BF16),
                *[pltpu.VMEM(s, BF16) for s in pairs],
                pltpu.SemaphoreType.DMA((3, 2)),
                pltpu.SemaphoreType.DMA((3, 2)),
                *sum_scratch(ep, width, last_lanes),
            ],
            4,
        )

    return jax.shard_map(body, mesh=mesh, in_specs=(tok_spec, tok_spec, route_spec, route_spec, repl_spec, exp_spec, exp_spec, exp_spec, repl_spec, repl_spec, repl_spec), out_specs=(tok_spec, repl_spec, exp_spec, exp_spec, exp_spec, repl_spec, repl_spec, repl_spec), check_vma=False)
```
